32 devices in a mesh: dp: 4 (over x, core), row: 2 (over y), col: 4 (over z).
Axes of the slice: x: 2, y: 2, z: 4, core: 2. Of those that a mesh axis runs over, the one named last changes fastest.
Arguments:
- act_in: bfloat16 [4096, 2304], P(('dp', 'row'), 'col'), may hold values from -6 to 6
- cot_out: bfloat16 [4096, 2304], P(('dp', 'row'), 'col'), may hold values from -6 to 6
- w_gate: bfloat16 [2304, 4608], P(('dp', 'row'), 'col'), may hold values from -0.125 to 0.125
- w_up: bfloat16 [2304, 4608], P(('dp', 'row'), 'col'), may hold values from -0.125 to 0.125
- w_down: bfloat16 [4608, 2304], P('col', ('dp', 'row')), may hold values from -0.09375 to 0.09375
Outputs:
- input_grad: bfloat16 [4096, 2304], P(('dp', 'row'), 'col')
- gate_grad: float32 [2304, 4608], P(('dp', 'row'), 'col')
- up_grad: float32 [2304, 4608], P(('dp', 'row'), 'col')
- down_grad: float32 [4608, 2304], P('col', ('dp', 'row'))
The draws below stay inside these ranges and needn't reach their ends.
All inputs are finite; a program needn't handle non-finite values.
Results may differ from the reference program's by a relative error of at most 0.015.
Values may be sent and summed in bfloat16 or wider, within the bound.
A program may use at most 128 MiB of HBM per device.

```python
import math
import jax
import jax.numpy as jnp
from jax import lax

D = 2304
FF = 4608
TOKENS = 4096
N_COL = 4


def with_spikes(result, key, source, target, shards_of, factor):
    def block_of(position):
        return (jnp.arange(result.shape[position]) // (result.shape[position] // shards_of)).reshape((-1,) + (1,) * (result.ndim - 1 - position))

    near = jax.random.permutation(key, shards_of)[block_of(target)]
    second = (block_of(target) + shards_of // 2) % shards_of
    return jnp.where((block_of(source) == near) | (block_of(source) == second), factor * result, result)


def levels(stream_key, dims, split, smallest, largest):
    loudness, own = 1.0, jax.random.fold_in(stream_key, 6)
    for dim, blocks in split:
        heights = jnp.exp(jax.random.uniform(jax.random.fold_in(own, dim), (blocks,), jnp.float32, smallest / len(split), largest / len(split)))
        loudness = loudness * jnp.repeat(heights, dims[dim] // blocks).reshape([-1 if axis == dim else 1 for axis in range(len(dims))])
    return loudness


def gaussian(rng, extent, deviation, reach, pieces=(), held_as=jnp.bfloat16):
    array = deviation * jax.random.normal(rng, extent, jnp.float32)
    if pieces:
        array = array * levels(rng, extent, pieces, -0.22, 0.18)
    return jnp.clip(array, -reach, reach).astype(held_as)


def heavy_noise(rng, extent, spread, bound, cuts, heavy, dtype=jnp.bfloat16):
    values = spread * jax.random.normal(rng, extent, jnp.float32)
    if cuts:
        values = values * levels(rng, extent, cuts, -0.22, 0.18)
    return jnp.clip(with_spikes(values, jax.random.fold_in(rng, 3), *heavy), -bound, bound).astype(dtype)


def setup_inputs(seed: int = 0) -> dict:
    splits = jax.random.split(jax.random.key(seed), 6)
    act_in = heavy_noise(splits[0], (TOKENS, D), 1.0, 6.0, ((0, 8), (1, 4)), (0, 1, 8, 2.0))
    cot_out = heavy_noise(splits[1], (TOKENS, D), 1.0, 6.0, ((0, 8), (1, 4)), (0, 1, 8, 2.0))
    w_gate = gaussian(splits[2], (D, FF), D ** -0.5, 0.125, ((0, 8), (1, 4)))
    w_up = gaussian(splits[3], (D, FF), D ** -0.5, 0.125, ((0, 8), (1, 4)))
    w_down = gaussian(splits[4], (FF, D), FF ** -0.5, 0.09375, ((0, 4), (1, 8)))
    return {"act_in": act_in, "cot_out": cot_out, "w_gate": w_gate, "w_up": w_up, "w_down": w_down}


gelu_cubic = 0.044715
gelu_scale = 0.7978845608028654

def gelu_parts(values):
    inner_arg = gelu_scale * (values + gelu_cubic * values * values * values)
    tanh_val = jnp.tanh(inner_arg)
    output = 0.5 * values * (1.0 + tanh_val)
    slope_val = 0.5 * (1.0 + tanh_val) + 0.5 * values * (1.0 - tanh_val * tanh_val) * gelu_scale * (1.0 + 3.0 * gelu_cubic * values * values)
    return (output, slope_val)

def reference(act_in, cot_out, w_gate, w_up, w_down):
    gate_pre = jnp.dot(act_in, w_gate, preferred_element_type=jnp.float32)
    up_pre = jnp.dot(act_in, w_up, preferred_element_type=jnp.float32)
    act_val, slope_val = gelu_parts(gate_pre)
    hidden = (act_val * up_pre).astype(jnp.bfloat16)
    hidden_grad = jnp.dot(cot_out, w_down.T, preferred_element_type=jnp.float32)
    d_gate = (hidden_grad * up_pre * slope_val).astype(jnp.bfloat16)
    d_up = (hidden_grad * act_val).astype(jnp.bfloat16)
    width = FF // N_COL
    input_sum = jnp.zeros(act_in.shape, jnp.float32)
    for column in range(N_COL):
        low_edge = column * width
        part_sum = jnp.dot(d_gate[:, low_edge:low_edge + width], w_gate[:, low_edge:low_edge + width].T, preferred_element_type=jnp.float32)
        part_sum = part_sum + jnp.dot(d_up[:, low_edge:low_edge + width], w_up[:, low_edge:low_edge + width].T, preferred_element_type=jnp.float32)
        input_sum = input_sum + lax.optimization_barrier(part_sum.astype(jnp.bfloat16)).astype(jnp.float32)
    input_grad = input_sum.astype(jnp.bfloat16)
    norm_scale = 1.0 / math.sqrt(TOKENS)
    gate_grad = jnp.dot(act_in.T, d_gate, preferred_element_type=jnp.float32) * norm_scale
    up_grad = jnp.dot(act_in.T, d_up, preferred_element_type=jnp.float32) * norm_scale
    down_grad = jnp.dot(hidden.T, cot_out, preferred_element_type=jnp.float32) * norm_scale
    return (input_grad, gate_grad, up_grad, down_grad)
```

```python
import functools
import math

import jax
import jax.numpy as jnp
from jax import lax
from jax.experimental import pallas as pl
from jax.experimental.pallas import tpu as pltpu
from jax.sharding import PartitionSpec as P

gelu_cubic = 0.044715
gelu_scale = 0.7978845608028654
MESH = pl.DeviceIdType.MESH
F32 = jnp.float32
BF16 = jnp.bfloat16


def gelu_parts(values):
    inner_arg = gelu_scale * (values + gelu_cubic * values * values * values)
    tanh_val = jnp.tanh(inner_arg)
    output = 0.5 * values * (1.0 + tanh_val)
    slope_val = 0.5 * (1.0 + tanh_val) + 0.5 * values * (1.0 - tanh_val * tanh_val) * gelu_scale * (
        1.0 + 3.0 * gelu_cubic * values * values
    )
    return (output, slope_val)


def tile_of(size, best):
    return best if size % best == 0 else size


def pieces_of(rows):
    if rows % 32 == 0:
        return [(0, 0, rows, 0), (1, 0, rows, 1), (2, 0, rows // 2, 0), (2, rows // 2, rows // 2, 1)]
    return [(0, 0, rows, 0), (1, 0, rows, 1), (2, 0, rows, 0)]


def others_first(n):
    return list(range(1, n)) + [0]


class Sends:
    def __init__(self, sems):
        self.sems, self.used, self.pending = sems, 0, []

    def start(self, src, dst, recv_sem, where, cond=None):
        copy = pltpu.make_async_remote_copy(
            src_ref=src,
            dst_ref=dst,
            send_sem=self.sems.at[self.used],
            recv_sem=recv_sem,
            device_id=where,
            device_id_type=MESH,
        )
        self.used += 1
        self.pending.append((cond, copy))
        guarded(cond, copy.start)

    def finish(self):
        for cond, copy in self.pending:
            guarded(cond, copy.wait_send)


def guarded(cond, action):
    if cond is None:
        action()
    else:
        pl.when(cond)(action)


def arrived(ref, sem):
    pltpu.make_async_copy(ref, ref, sem).wait()


def kernel(sizes, act_ref, cot_ref, wg_ref, wu_ref, wd_ref, ig_ref, og_ref, ou_ref, od_ref,
           full, weights, grads, stash, partner_out, sums, first_in, second_in, ig_out, ig_in,
           own_sem, send_sem, w_sem, x_sem, pair_send, pair_recv, first_sem, second_sem, ig_sem):
    n_dp, n_row, n_col, rows, hid, feats, toks = sizes
    nq, ny = n_dp // 2, n_row
    peers = nq * ny
    pieces = pieces_of(rows)
    dp, y, col = lax.axis_index("dp"), lax.axis_index("row"), lax.axis_index("col")
    q, c = dp // 2, dp % 2
    rep_of = lambda q1, c1, y1: (q1 * 2 + c1) * ny + y1
    at_q = lambda dq: lax.rem(q + dq, nq)
    at_y = lambda dy: lax.rem(y + dy, ny)
    back_q = lambda dq: lax.rem(q + nq - dq, nq)
    back_y = lambda dy: lax.rem(y + ny - dy, ny)
    me = rep_of(q, c, y)
    partner = {"dp": q * 2 + 1 - c}
    q_peer = lambda dq: {"dp": at_q(dq) * 2 + c}
    y_peer = lambda dy: {"row": at_y(dy)}

    barrier = pltpu.get_barrier_semaphore()
    friends = [partner] + [q_peer(i) for i in range(1, nq)] + [y_peer(i) for i in range(1, ny)]
    friends += [{"col": lax.rem(col + i, n_col)} for i in range(1, n_col)]
    for friend in friends:
        pl.semaphore_signal(barrier, inc=1, device_id=friend, device_id_type=MESH)
    pl.semaphore_wait(barrier, len(friends))

    sends = Sends(send_sem)
    mine = (wg_ref, wu_ref, wd_ref)
    streams = (act_ref, cot_ref)

    def rows_at(rep, r0, nr):
        return pl.ds(pl.multiple_of(rep * rows + r0, 8), nr)

    def slot(p, rep):
        w, r0, nr, _ = pieces[p]
        return weights.at[w, rows_at(rep, r0, nr), :]

    def feat_slot(s, block):
        return full.at[s, pl.ds(pl.multiple_of(block * feats, 8), feats), :]

    has_right, has_left = col < n_col - 1, col > 0
    right = {"col": jnp.minimum(col + 1, n_col - 1)}
    left = {"col": jnp.maximum(col - 1, 0)}
    for s in range(2):
        sends.start(streams[s], feat_slot(s, col), x_sem.at[s * n_col + col], right, has_right)
        sends.start(streams[s], feat_slot(s, col), x_sem.at[s * n_col + col], left, has_left)
    for p, (w, r0, nr, route) in enumerate(pieces):
        src = mine[w].at[pl.ds(r0, nr), :]
        sem = w_sem.at[p * peers * 2 + me]
        for dq in range(1, nq):
            sends.start(src, slot(p, me), sem, q_peer(dq))
        for dy in range(1, ny):
            sends.start(src, slot(p, me), sem, y_peer(dy))
        sends.start(src, slot(p, me), sem, partner)
    locals_ = []
    for i, (src, dst) in enumerate(
        [(streams[s], feat_slot(s, col)) for s in range(2)]
        + [(mine[w], weights.at[w, rows_at(me, 0, rows), :]) for w in range(3)]
    ):
        locals_.append(pltpu.make_async_copy(src, dst, own_sem.at[i]))
        locals_[-1].start()

    def chain(s, step):
        from_left, from_right = col >= step, col + step < n_col
        lb, rb = jnp.maximum(col - step, 0), jnp.minimum(col + step, n_col - 1)
        l_sem, r_sem = x_sem.at[s * n_col + lb], x_sem.at[s * n_col + rb]
        guarded(from_left, lambda: arrived(feat_slot(s, lb), l_sem))
        if step < n_col - 1:
            sends.start(feat_slot(s, lb), feat_slot(s, lb), l_sem, right, from_left & has_right)
        guarded(from_right, lambda: arrived(feat_slot(s, rb), r_sem))
        if step < n_col - 1:
            sends.start(feat_slot(s, rb), feat_slot(s, rb), r_sem, left, from_right & has_left)

    def take(p, rep, forward):
        sem = w_sem.at[p * peers * 2 + rep]
        arrived(slot(p, rep), sem)
        for where in forward + [partner]:
            sends.start(slot(p, rep), slot(p, rep), sem, where)

    def near(p):
        route = pieces[p][3]
        for dq in range(1, nq):
            take(p, rep_of(back_q(dq), c, y), [y_peer(i) for i in range(1, ny)] if route == 0 else [])
        for dy in range(1, ny):
            take(p, rep_of(q, c, back_y(dy)), [q_peer(i) for i in range(1, nq)] if route == 1 else [])

    def far(p):
        for dq in range(1, nq):
            for dy in range(1, ny):
                take(p, rep_of(back_q(dq), c, back_y(dy)), [])

    def from_partner(p):
        for dq in range(nq):
            for dy in range(ny):
                rep = rep_of(at_q(dq), 1 - c, at_y(dy))
                arrived(slot(p, rep), w_sem.at[p * peers * 2 + rep])

    todo = [functools.partial(near, p) for p in range(len(pieces))]
    todo += [functools.partial(far, p) for p in range(len(pieces))]
    chains = [functools.partial(chain, s, step) for step in range(1, n_col) for s in range(2)]
    while len(chains) > 1 or todo:
        if len(chains) > 1:
            chains.pop(0)()
        if todo:
            todo.pop(0)()
    for p in range(len(pieces)):
        from_partner(p)
    for copy in locals_:
        copy.wait()

    mt, nt = tile_of(toks, 256), tile_of(hid, 384)
    m_tiles, n_tiles = toks // mt, hid // nt
    token_dims = (((0,), (0,)), ((), ()))

    def tile_slices(i):
        m, n = i // n_tiles, i % n_tiles
        return pl.ds(pl.multiple_of(m * mt, mt), mt), pl.ds(pl.multiple_of(n * nt, nt), nt)

    @pl.loop(0, m_tiles * n_tiles)
    def _(i):
        ms, ns = tile_slices(i)
        x = full[0, :, ms]
        gate_pre = lax.dot_general(x, weights[0, :, ns], token_dims, preferred_element_type=F32)
        up_pre = lax.dot_general(x, weights[1, :, ns], token_dims, preferred_element_type=F32)
        act_val, slope_val = gelu_parts(gate_pre)
        grads[2, ms, ns] = (act_val * up_pre).astype(BF16)
        stash[0, ms, ns] = up_pre * slope_val
        stash[1, ms, ns] = act_val

    chains.pop(0)()

    @pl.loop(0, m_tiles * n_tiles)
    def _(i):
        ms, ns = tile_slices(i)
        hidden_grad = lax.dot_general(full[1, :, ms], weights[2, :, ns], token_dims, preferred_element_type=F32)
        grads[0, ms, ns] = (hidden_grad * stash[0, ms, ns]).astype(BF16)
        grads[1, ms, ns] = (hidden_grad * stash[1, ms, ns]).astype(BF16)

    def term(w, rep, ns):
        return jnp.dot(full[w // 2, rows_at(rep, 0, rows), :], grads[w, :, ns], preferred_element_type=F32)

    def n_slice(n):
        return pl.ds(pl.multiple_of(n * nt, nt), nt)

    def pair_copy(i):
        return pltpu.make_async_remote_copy(
            src_ref=partner_out.at[i],
            dst_ref=sums.at[i],
            send_sem=pair_send.at[i],
            recv_sem=pair_recv.at[i],
            device_id=partner,
            device_id_type=MESH,
        )

    @pl.loop(0, 3 * peers)
    def _(i):
        w, peer = i // peers, i % peers
        rep = rep_of(peer // ny, 1 - c, peer % ny)

        @pl.loop(0, n_tiles)
        def _(n):
            partner_out[i, :, n_slice(n)] = term(w, rep, n_slice(n)).astype(BF16)

        pair_copy(i).start()

    first_base, count = [], 0
    for _, _, _, route in pieces:
        first_base.append(count)
        count += (nq - 1) * ny if route == 0 else (ny - 1) * nq
    second_base, count = [], 0
    for _, _, _, route in pieces:
        second_base.append(count)
        count += (ny - 1) if route == 0 else (nq - 1)

    def first_slot(p, dq, dy):
        k = first_base[p] + ((dq - 1) * ny + dy if pieces[p][3] == 0 else (dy - 1) * nq + dq)
        return first_in.at[k, pl.ds(0, pieces[p][2]), :], first_sem.at[k]

    def second_slot(p, d):
        k = second_base[p] + d - 1
        return second_in.at[k, pl.ds(0, pieces[p][2]), :], second_sem.at[k]

    for w in range(3):
        for dq in others_first(nq):
            for dy in others_first(ny):
                index = w * peers + at_q(dq) * ny + at_y(dy)
                rep = rep_of(at_q(dq), c, at_y(dy))
                arrived(sums.at[index], pair_recv.at[index])

                @pl.loop(0, n_tiles)
                def _(n):
                    ns = n_slice(n)
                    sums[index, :, ns] = (term(w, rep, ns) + sums[index, :, ns].astype(F32)).astype(BF16)

                for p, (pw, r0, nr, route) in enumerate(pieces):
                    if pw == w and (dq if route == 0 else dy):
                        dst, sem = first_slot(p, dq, dy)
                        where = q_peer(dq) if route == 0 else y_peer(dy)
                        sends.start(sums.at[index, pl.ds(r0, nr), :], dst, sem, where)

    rt = tile_of(feats, 288)
    hid_dims = (((1,), (1,)), ((), ()))
    for dz in others_first(n_col):
        block = lax.rem(col + dz, n_col)

        @pl.loop(0, feats // rt)
        def _(r):
            rs = pl.ds(pl.multiple_of(block * feats + r * rt, 8), rt)
            part = lax.dot_general(weights[0, rs, :], grads[0], hid_dims, preferred_element_type=F32)
            part = part + lax.dot_general(weights[1, rs, :], grads[1], hid_dims, preferred_element_type=F32)
            ig_out[dz, pl.ds(pl.multiple_of(r * rt, 8), rt), :] = part.astype(BF16)

        if dz:
            sends.start(ig_out.at[dz], ig_in.at[dz - 1], ig_sem.at[dz - 1], {"col": block})

    outs = (og_ref, ou_ref, od_ref)
    for p, (w, r0, nr, route) in enumerate(pieces):
        rs = pl.ds(r0, nr)
        n_first, n_second = (nq, ny) if route == 0 else (ny, nq)
        for d in others_first(n_second):
            index = w * peers + (q * ny + at_y(d) if route == 0 else at_q(d) * ny + y)
            total = sums[index, rs, :].astype(F32)
            for f in range(1, n_first):
                ref, sem = first_slot(p, f, d) if route == 0 else first_slot(p, d, f)
                arrived(ref, sem)
                total = total + ref[...].astype(F32)
            if d:
                sums[index, rs, :] = total.astype(BF16)
                dst, sem = second_slot(p, d)
                sends.start(sums.at[index, rs, :], dst, sem, y_peer(d) if route == 0 else q_peer(d))
            else:
                outs[w][rs, :] = total

    total = ig_out[0].astype(F32)
    for dz in range(1, n_col):
        arrived(ig_in.at[dz - 1], ig_sem.at[dz - 1])
        total = total + ig_in[dz - 1].astype(F32)
    ig_ref[...] = total.astype(BF16)

    for p, (w, r0, nr, route) in enumerate(pieces):
        rs = pl.ds(r0, nr)
        for d in range(1, ny if route == 0 else nq):
            ref, sem = second_slot(p, d)
            arrived(ref, sem)
            outs[w][rs, :] = outs[w][rs, :] + ref[...].astype(F32)

    sends.finish()

    @pl.loop(0, 3 * peers)
    def _(i):
        pair_copy(i).wait_send()


def body(n_dp, n_row, n_col, act_in, cot_out, w_gate, w_up, w_down):
    toks, feats = act_in.shape
    rows, hid = w_gate.shape
    sizes = (n_dp, n_row, n_col, rows, hid, feats, toks)
    nq, ny = n_dp // 2, n_row
    peers, reps, dim = nq * ny, n_dp * n_row, feats * n_col
    pieces = pieces_of(rows)
    firsts = sum((nq - 1) * ny if r == 0 else (ny - 1) * nq for _, _, _, r in pieces)
    seconds = sum((ny - 1) if r == 0 else (nq - 1) for _, _, _, r in pieces)
    near_far = sum((nq - 1) * (ny - 1) for _ in pieces)
    n_sends = 4 + 4 * (n_col - 2) + len(pieces) * (nq + ny - 1) + len(pieces) * (peers - 1) + near_far
    n_sends += firsts + seconds + n_col - 1
    any_spec, vmem_spec = pl.BlockSpec(memory_space=pl.ANY), pl.BlockSpec(memory_space=pltpu.VMEM)
    dma = lambda n: pltpu.SemaphoreType.DMA((max(n, 1),))
    wgrad = jax.ShapeDtypeStruct((rows, hid), F32)
    ig_t, gate_grad, up_grad, down_t = pl.pallas_call(
        functools.partial(kernel, sizes),
        out_shape=[jax.ShapeDtypeStruct((feats, toks), BF16), wgrad, wgrad, wgrad],
        in_specs=[any_spec] * 5,
        out_specs=[vmem_spec] * 4,
        scratch_shapes=[
            pltpu.VMEM((2, dim, toks), BF16),
            pltpu.VMEM((3, dim, hid), BF16),
            pltpu.VMEM((3, toks, hid), BF16),
            pltpu.VMEM((2, toks, hid), F32),
            pltpu.VMEM((3 * peers, rows, hid), BF16),
            pltpu.VMEM((3 * peers, rows, hid), BF16),
            pltpu.VMEM((max(firsts, 1), rows, hid), BF16),
            pltpu.VMEM((max(seconds, 1), rows, hid), BF16),
            pltpu.VMEM((n_col, feats, toks), BF16),
            pltpu.VMEM((max(n_col - 1, 1), feats, toks), BF16),
            dma(5), dma(n_sends), dma(len(pieces) * reps), dma(2 * n_col), dma(3 * peers), dma(3 * peers),
            dma(firsts), dma(seconds), dma(n_col - 1),
        ],
        compiler_params=pltpu.CompilerParams(
            collective_id=0, has_side_effects=True, vmem_limit_bytes=67043328
        ),
    )(act_in.T, cot_out.T, w_gate, w_up, w_down.T)
    norm_scale = 1.0 / math.sqrt(toks * n_dp * n_row)
    return (ig_t.T, gate_grad * norm_scale, up_grad * norm_scale, (down_t * norm_scale).T)


def solution(mesh):
    grid = P(("dp", "row"), "col")
    flipped = P("col", ("dp", "row"))
    return jax.shard_map(
        functools.partial(body, mesh.shape["dp"], mesh.shape["row"], mesh.shape["col"]),
        mesh=mesh,
        in_specs=(grid, grid, grid, grid, flipped),
        out_specs=(grid, grid, grid, flipped),
        check_vma=False,
    )
```

```python
import functools
import math

import jax
import jax.numpy as jnp
from jax import lax
from jax.experimental import pallas as pl
from jax.experimental.pallas import tpu as pltpu
from jax.sharding import PartitionSpec as P

gelu_cubic = 0.044715
gelu_scale = 0.7978845608028654
MESH = pl.DeviceIdType.MESH
F32 = jnp.float32
BF16 = jnp.bfloat16


def gelu_parts(values):
    inner_arg = gelu_scale * (values + gelu_cubic * values * values * values)
    tanh_val = jnp.tanh(inner_arg)
    output = 0.5 * values * (1.0 + tanh_val)
    slope_val = 0.5 * (1.0 + tanh_val) + 0.5 * values * (1.0 - tanh_val * tanh_val) * gelu_scale * (
        1.0 + 3.0 * gelu_cubic * values * values
    )
    return (output, slope_val)


def tile_of(size, best):
    return best if size % best == 0 else size


def pieces_of(rows):
    if rows % 32 == 0:
        return [(0, 0, rows, 0), (1, 0, rows, 1), (2, 0, rows // 2, 0), (2, rows // 2, rows // 2, 1)]
    return [(0, 0, rows, 0), (1, 0, rows, 1), (2, 0, rows, 0)]


def others_first(n):
    return list(range(1, n)) + [0]


class Sends:
    def __init__(self, sems):
        self.sems, self.used, self.pending = sems, 0, []

    def start(self, src, dst, recv_sem, where, cond=None):
        copy = pltpu.make_async_remote_copy(
            src_ref=src,
            dst_ref=dst,
            send_sem=self.sems.at[self.used],
            recv_sem=recv_sem,
            device_id=where,
            device_id_type=MESH,
        )
        self.used += 1
        self.pending.append((cond, copy))
        guarded(cond, copy.start)

    def finish(self):
        for cond, copy in self.pending:
            guarded(cond, copy.wait_send)


def guarded(cond, action):
    if cond is None:
        action()
    else:
        pl.when(cond)(action)


def arrived(ref, sem):
    pltpu.make_async_copy(ref, ref, sem).wait()


def kernel(sizes, act_ref, cot_ref, wg_ref, wu_ref, wd_ref, ig_ref, og_ref, ou_ref, od_ref,
           full, weights, grads, stash, partner_out, sums, first_in, second_in, ig_out, ig_in,
           own_sem, send_sem, w_sem, x_sem, pair_send, pair_recv, first_sem, second_sem, ig_sem):
    n_dp, n_row, n_col, rows, hid, feats, toks = sizes
    nq, ny = n_dp // 2, n_row
    peers = nq * ny
    pieces = pieces_of(rows)
    dp, y, col = lax.axis_index("dp"), lax.axis_index("row"), lax.axis_index("col")
    q, c = dp // 2, dp % 2
    rep_of = lambda q1, c1, y1: (q1 * 2 + c1) * ny + y1
    at_q = lambda dq: lax.rem(q + dq, nq)
    at_y = lambda dy: lax.rem(y + dy, ny)
    back_q = lambda dq: lax.rem(q + nq - dq, nq)
    back_y = lambda dy: lax.rem(y + ny - dy, ny)
    me = rep_of(q, c, y)
    partner = {"dp": q * 2 + 1 - c}
    q_peer = lambda dq: {"dp": at_q(dq) * 2 + c}
    y_peer = lambda dy: {"row": at_y(dy)}

    barrier = pltpu.get_barrier_semaphore()
    friends = [partner] + [q_peer(i) for i in range(1, nq)] + [y_peer(i) for i in range(1, ny)]
    friends += [{"col": lax.rem(col + i, n_col)} for i in range(1, n_col)]
    for friend in friends:
        pl.semaphore_signal(barrier, inc=1, device_id=friend, device_id_type=MESH)
    pl.semaphore_wait(barrier, len(friends))

    sends = Sends(send_sem)
    mine = (wg_ref, wu_ref, wd_ref)
    streams = (act_ref, cot_ref)

    def rows_at(rep, r0, nr):
        return pl.ds(pl.multiple_of(rep * rows + r0, 8), nr)

    def slot(p, rep):
        w, r0, nr, _ = pieces[p]
        return weights.at[w, rows_at(rep, r0, nr), :]

    half = feats // 2

    def feat_slot(s, h, block):
        return full.at[s, pl.ds(pl.multiple_of(block * feats + h * half, 8), half), :]

    def feat_sem(s, h, block):
        return x_sem.at[(s * 2 + h) * n_col + block]

    has_right, has_left = col < n_col - 1, col > 0
    right = {"col": jnp.minimum(col + 1, n_col - 1)}
    left = {"col": jnp.maximum(col - 1, 0)}

    def own_features(s):
        for h in range(2):
            src = streams[s].at[pl.ds(h * half, half), :]
            sends.start(src, feat_slot(s, h, col), feat_sem(s, h, col), right, has_right)
            sends.start(src, feat_slot(s, h, col), feat_sem(s, h, col), left, has_left)

    def own_weight(weight):
        for p, (w, r0, nr, route) in enumerate(pieces):
            if w != weight:
                continue
            src = mine[w].at[pl.ds(r0, nr), :]
            sem = w_sem.at[p * peers * 2 + me]
            for dq in range(1, nq):
                sends.start(src, slot(p, me), sem, q_peer(dq))
            for dy in range(1, ny):
                sends.start(src, slot(p, me), sem, y_peer(dy))
            sends.start(src, slot(p, me), sem, partner)

    own_features(0)
    own_weight(0)
    own_weight(1)
    locals_ = []
    for i, (src, dst) in enumerate(
        [(streams[s], full.at[s, pl.ds(pl.multiple_of(col * feats, 8), feats), :]) for s in range(2)]
        + [(mine[w], weights.at[w, rows_at(me, 0, rows), :]) for w in range(3)]
    ):
        locals_.append(pltpu.make_async_copy(src, dst, own_sem.at[i]))
        locals_[-1].start()

    def chain(s, step):
        from_left, from_right = col >= step, col + step < n_col
        lb, rb = jnp.maximum(col - step, 0), jnp.minimum(col + step, n_col - 1)
        for h in range(2):
            l_slot, l_sem = feat_slot(s, h, lb), feat_sem(s, h, lb)
            r_slot, r_sem = feat_slot(s, h, rb), feat_sem(s, h, rb)
            guarded(from_left, lambda: arrived(l_slot, l_sem))
            if step < n_col - 1:
                sends.start(l_slot, l_slot, l_sem, right, from_left & has_right)
            guarded(from_right, lambda: arrived(r_slot, r_sem))
            if step < n_col - 1:
                sends.start(r_slot, r_slot, r_sem, left, from_right & has_left)

    def take(p, rep, forward):
        sem = w_sem.at[p * peers * 2 + rep]
        arrived(slot(p, rep), sem)
        for where in forward + [partner]:
            sends.start(slot(p, rep), slot(p, rep), sem, where)

    def near(p):
        route = pieces[p][3]
        for dq in range(1, nq):
            take(p, rep_of(back_q(dq), c, y), [y_peer(i) for i in range(1, ny)] if route == 0 else [])
        for dy in range(1, ny):
            take(p, rep_of(q, c, back_y(dy)), [q_peer(i) for i in range(1, nq)] if route == 1 else [])

    def far(p):
        for dq in range(1, nq):
            for dy in range(1, ny):
                take(p, rep_of(back_q(dq), c, back_y(dy)), [])

    def from_partner(p):
        for dq in range(nq):
            for dy in range(ny):
                rep = rep_of(at_q(dq), 1 - c, at_y(dy))
                arrived(slot(p, rep), w_sem.at[p * peers * 2 + rep])

    near(0)
    chain(0, 1)
    near(1)
    own_weight(2)
    for step in range(2, n_col):
        if step == n_col - 1:
            own_features(1)
        chain(0, step)
    far(0)
    far(1)
    from_partner(0)
    from_partner(1)
    for copy in locals_:
        copy.wait()

    mt, nt = tile_of(toks, 256), tile_of(hid, 384)
    m_tiles, n_tiles = toks // mt, hid // nt
    token_dims = (((0,), (0,)), ((), ()))
    later = [p for p in range(len(pieces)) if pieces[p][0] == 2]

    def tile_slices(i):
        m, n = i // n_tiles, i % n_tiles
        return pl.ds(pl.multiple_of(m * mt, mt), mt), pl.ds(pl.multiple_of(n * nt, nt), nt)

    def project(first, last):
        @pl.loop(first, last)
        def _(i):
            ms, ns = tile_slices(i)
            x = full[0, :, ms]
            gate_pre = lax.dot_general(x, weights[0, :, ns], token_dims, preferred_element_type=F32)
            up_pre = lax.dot_general(x, weights[1, :, ns], token_dims, preferred_element_type=F32)
            act_val, slope_val = gelu_parts(gate_pre)
            grads[2, ms, ns] = (act_val * up_pre).astype(BF16)
            stash[0, ms, ns] = up_pre * slope_val
            stash[1, ms, ns] = act_val

    tiles = m_tiles * n_tiles
    project(0, tiles // 2)
    chain(1, 1)
    project(tiles // 2, tiles)
    for p in later:
        near(p)
    for step in range(2, n_col - 1):
        chain(1, step)

    def term(w, rep, ns):
        return jnp.dot(full[w // 2, rows_at(rep, 0, rows), :], grads[w, :, ns], preferred_element_type=F32)

    def n_slice(n):
        return pl.ds(pl.multiple_of(n * nt, nt), nt)

    def pair_copy(i):
        return pltpu.make_async_remote_copy(
            src_ref=partner_out.at[i],
            dst_ref=sums.at[i],
            send_sem=pair_send.at[i],
            recv_sem=pair_recv.at[i],
            device_id=partner,
            device_id_type=MESH,
        )

    def is_far(rep):
        block = (rep * rows) // feats
        return jnp.abs(block - col) == n_col - 1

    def partner_terms(w, when=None):
        @pl.loop(0, peers)
        def _(peer):
            i = w * peers + peer
            rep = rep_of(peer // ny, 1 - c, peer % ny)

            def one():
                @pl.loop(0, n_tiles)
                def _(n):
                    partner_out[i, :, n_slice(n)] = term(w, rep, n_slice(n)).astype(BF16)

                pair_copy(i).start()

            guarded(None if when is None else when(rep), one)

    first_base, count = [], 0
    for _, _, _, route in pieces:
        first_base.append(count)
        count += (nq - 1) * ny if route == 0 else (ny - 1) * nq
    second_base, count = [], 0
    for _, _, _, route in pieces:
        second_base.append(count)
        count += (ny - 1) if route == 0 else (nq - 1)

    def first_slot(p, dq, dy):
        k = first_base[p] + ((dq - 1) * ny + dy if pieces[p][3] == 0 else (dy - 1) * nq + dq)
        return first_in.at[k, pl.ds(0, pieces[p][2]), :], first_sem.at[k]

    def second_slot(p, d):
        k = second_base[p] + d - 1
        return second_in.at[k, pl.ds(0, pieces[p][2]), :], second_sem.at[k]

    def own_terms(w, when=None):
        for dq in others_first(nq):
            for dy in others_first(ny):
                index = w * peers + at_q(dq) * ny + at_y(dy)
                rep = rep_of(at_q(dq), c, at_y(dy))
                cond = None if when is None else when(rep)

                def one():
                    arrived(sums.at[index], pair_recv.at[index])

                    @pl.loop(0, n_tiles)
                    def _(n):
                        ns = n_slice(n)
                        sums[index, :, ns] = (term(w, rep, ns) + sums[index, :, ns].astype(F32)).astype(BF16)

                guarded(cond, one)
                for p, (pw, r0, nr, route) in enumerate(pieces):
                    if pw == w and (dq if route == 0 else dy):
                        dst, sem = first_slot(p, dq, dy)
                        where = q_peer(dq) if route == 0 else y_peer(dy)
                        sends.start(sums.at[index, pl.ds(r0, nr), :], dst, sem, where, cond)

    rt = tile_of(feats, 288)
    hid_dims = (((1,), (1,)), ((), ()))

    def input_part(dz):
        block = lax.rem(col + dz, n_col)

        @pl.loop(0, feats // rt)
        def _(r):
            rs = pl.ds(pl.multiple_of(block * feats + r * rt, 8), rt)
            part = lax.dot_general(weights[0, rs, :], grads[0], hid_dims, preferred_element_type=F32)
            part = part + lax.dot_general(weights[1, rs, :], grads[1], hid_dims, preferred_element_type=F32)
            ig_out[dz, pl.ds(pl.multiple_of(r * rt, 8), rt), :] = part.astype(BF16)

        if dz:
            sends.start(ig_out.at[dz], ig_in.at[dz - 1], ig_sem.at[dz - 1], {"col": block})

    outs = (og_ref, ou_ref, od_ref)

    def second(p):
        w, r0, nr, route = pieces[p]
        rs = pl.ds(r0, nr)
        n_first, n_second = (nq, ny) if route == 0 else (ny, nq)
        for d in others_first(n_second):
            index = w * peers + (q * ny + at_y(d) if route == 0 else at_q(d) * ny + y)
            total = sums[index, rs, :].astype(F32)
            for f in range(1, n_first):
                ref, sem = first_slot(p, f, d) if route == 0 else first_slot(p, d, f)
                arrived(ref, sem)
                total = total + ref[...].astype(F32)
            if d:
                sums[index, rs, :] = total.astype(BF16)
                dst, sem = second_slot(p, d)
                sends.start(sums.at[index, rs, :], dst, sem, y_peer(d) if route == 0 else q_peer(d))
            else:
                outs[w][rs, :] = total

    near_rep = lambda rep: jnp.logical_not(is_far(rep))
    partner_terms(2, near_rep)
    own_terms(2, near_rep)
    for p in later:
        far(p)
    for p in later:
        from_partner(p)
    chain(1, n_col - 1)
    partner_terms(2, is_far)

    @pl.loop(0, tiles)
    def _(i):
        ms, ns = tile_slices(i)
        hidden_grad = lax.dot_general(full[1, :, ms], weights[2, :, ns], token_dims, preferred_element_type=F32)
        grads[0, ms, ns] = (hidden_grad * stash[0, ms, ns]).astype(BF16)
        grads[1, ms, ns] = (hidden_grad * stash[1, ms, ns]).astype(BF16)

    own_terms(2, is_far)
    spare = list(range(1, n_col))
    partner_terms(0)
    input_part(spare.pop(0))
    own_terms(0)
    if spare:
        input_part(spare.pop(0))
    partner_terms(1)
    for p in later:
        second(p)
    while spare:
        input_part(spare.pop(0))
    own_terms(1)
    input_part(0)
    for p in range(len(pieces)):
        if p not in later:
            second(p)

    total = ig_out[0].astype(F32)
    for dz in range(1, n_col):
        arrived(ig_in.at[dz - 1], ig_sem.at[dz - 1])
        total = total + ig_in[dz - 1].astype(F32)
    ig_ref[...] = total.astype(BF16)

    for p, (w, r0, nr, route) in enumerate(pieces):
        rs = pl.ds(r0, nr)
        for d in range(1, ny if route == 0 else nq):
            ref, sem = second_slot(p, d)
            arrived(ref, sem)
            outs[w][rs, :] = outs[w][rs, :] + ref[...].astype(F32)

    sends.finish()

    @pl.loop(0, 3 * peers)
    def _(i):
        pair_copy(i).wait_send()


def body(n_dp, n_row, n_col, act_in, cot_out, w_gate, w_up, w_down):
    toks, feats = act_in.shape
    rows, hid = w_gate.shape
    sizes = (n_dp, n_row, n_col, rows, hid, feats, toks)
    nq, ny = n_dp // 2, n_row
    peers, reps, dim = nq * ny, n_dp * n_row, feats * n_col
    pieces = pieces_of(rows)
    firsts = sum((nq - 1) * ny if r == 0 else (ny - 1) * nq for _, _, _, r in pieces)
    seconds = sum((ny - 1) if r == 0 else (nq - 1) for _, _, _, r in pieces)
    near_far = sum((nq - 1) * (ny - 1) for _ in pieces)
    n_sends = 8 + 8 * (n_col - 2) + len(pieces) * (nq + ny - 1) + len(pieces) * (peers - 1) + near_far
    n_sends += 2 * firsts + seconds + n_col - 1
    any_spec, vmem_spec = pl.BlockSpec(memory_space=pl.ANY), pl.BlockSpec(memory_space=pltpu.VMEM)
    dma = lambda n: pltpu.SemaphoreType.DMA((max(n, 1),))
    wgrad = jax.ShapeDtypeStruct((rows, hid), F32)
    ig_t, gate_grad, up_grad, down_t = pl.pallas_call(
        functools.partial(kernel, sizes),
        out_shape=[jax.ShapeDtypeStruct((feats, toks), BF16), wgrad, wgrad, wgrad],
        in_specs=[any_spec] * 5,
        out_specs=[vmem_spec] * 4,
        scratch_shapes=[
            pltpu.VMEM((2, dim, toks), BF16),
            pltpu.VMEM((3, dim, hid), BF16),
            pltpu.VMEM((3, toks, hid), BF16),
            pltpu.VMEM((2, toks, hid), F32),
            pltpu.VMEM((3 * peers, rows, hid), BF16),
            pltpu.VMEM((3 * peers, rows, hid), BF16),
            pltpu.VMEM((max(firsts, 1), rows, hid), BF16),
            pltpu.VMEM((max(seconds, 1), rows, hid), BF16),
            pltpu.VMEM((n_col, feats, toks), BF16),
            pltpu.VMEM((max(n_col - 1, 1), feats, toks), BF16),
            dma(5), dma(n_sends), dma(len(pieces) * reps), dma(4 * n_col), dma(3 * peers), dma(3 * peers),
            dma(firsts), dma(seconds), dma(n_col - 1),
        ],
        compiler_params=pltpu.CompilerParams(
            collective_id=0, has_side_effects=True, vmem_limit_bytes=67043328
        ),
    )(act_in.T, cot_out.T, w_gate, w_up, w_down.T)
    norm_scale = 1.0 / math.sqrt(toks * n_dp * n_row)
    return (ig_t.T, gate_grad * norm_scale, up_grad * norm_scale, (down_t * norm_scale).T)


def solution(mesh):
    grid = P(("dp", "row"), "col")
    flipped = P("col", ("dp", "row"))
    return jax.shard_map(
        functools.partial(body, mesh.shape["dp"], mesh.shape["row"], mesh.shape["col"]),
        mesh=mesh,
        in_specs=(grid, grid, grid, grid, flipped),
        out_specs=(grid, grid, grid, flipped),
        check_vma=False,
    )
```

```python
import functools
import math

import jax
import jax.numpy as jnp
from jax import lax
from jax.experimental import pallas as pl
from jax.experimental.pallas import tpu as pltpu
from jax.sharding import PartitionSpec as P

gelu_cubic = 0.044715
gelu_scale = 0.7978845608028654
MESH = pl.DeviceIdType.MESH
F32 = jnp.float32
BF16 = jnp.bfloat16


def gelu_parts(values):
    inner_arg = gelu_scale * (values + gelu_cubic * values * values * values)
    tanh_val = jnp.tanh(inner_arg)
    output = 0.5 * values * (1.0 + tanh_val)
    slope_val = 0.5 * (1.0 + tanh_val) + 0.5 * values * (1.0 - tanh_val * tanh_val) * gelu_scale * (
        1.0 + 3.0 * gelu_cubic * values * values
    )
    return (output, slope_val)


def tile_of(size, best):
    return best if size % best == 0 else size


def pieces_of(rows):
    if rows % 32 == 0:
        return [(0, 0, rows, 0), (1, 0, rows, 1), (2, 0, rows // 2, 0), (2, rows // 2, rows // 2, 1)]
    return [(0, 0, rows, 0), (1, 0, rows, 1), (2, 0, rows, 0)]


def others_first(n):
    return list(range(1, n)) + [0]


class Sends:
    def __init__(self, sems):
        self.sems, self.used, self.pending = sems, 0, []

    def start(self, src, dst, recv_sem, where, cond=None):
        copy = pltpu.make_async_remote_copy(
            src_ref=src,
            dst_ref=dst,
            send_sem=self.sems.at[self.used],
            recv_sem=recv_sem,
            device_id=where,
            device_id_type=MESH,
        )
        self.used += 1
        self.pending.append((cond, copy))
        guarded(cond, copy.start)

    def finish(self):
        for cond, copy in self.pending:
            guarded(cond, copy.wait_send)


def guarded(cond, action):
    if cond is None:
        action()
    else:
        pl.when(cond)(action)


def arrived(ref, sem):
    pltpu.make_async_copy(ref, ref, sem).wait()


def kernel(sizes, act_ref, cot_ref, wg_ref, wu_ref, wd_ref, ig_ref, og_ref, ou_ref, od_ref,
           full, weights, grads, stash, partner_out, sums, first_in, second_in, ig_out, ig_in,
           own_sem, send_sem, w_sem, x_sem, pair_send, pair_recv, first_sem, second_sem, ig_sem):
    n_dp, n_row, n_col, rows, hid, feats, toks = sizes
    nq, ny = n_dp // 2, n_row
    peers = nq * ny
    pieces = pieces_of(rows)
    dp, y, col = lax.axis_index("dp"), lax.axis_index("row"), lax.axis_index("col")
    q, c = dp // 2, dp % 2
    rep_of = lambda q1, c1, y1: (q1 * 2 + c1) * ny + y1
    at_q = lambda dq: lax.rem(q + dq, nq)
    at_y = lambda dy: lax.rem(y + dy, ny)
    back_q = lambda dq: lax.rem(q + nq - dq, nq)
    back_y = lambda dy: lax.rem(y + ny - dy, ny)
    me = rep_of(q, c, y)
    partner = {"dp": q * 2 + 1 - c}
    q_peer = lambda dq: {"dp": at_q(dq) * 2 + c}
    y_peer = lambda dy: {"row": at_y(dy)}

    barrier = pltpu.get_barrier_semaphore()
    friends = [partner] + [q_peer(i) for i in range(1, nq)] + [y_peer(i) for i in range(1, ny)]
    friends += [{"col": lax.rem(col + i, n_col)} for i in range(1, n_col)]
    for friend in friends:
        pl.semaphore_signal(barrier, inc=1, device_id=friend, device_id_type=MESH)
    pl.semaphore_wait(barrier, len(friends))

    sends = Sends(send_sem)
    mine = (wg_ref, wu_ref, wd_ref)
    streams = (act_ref, cot_ref)

    def rows_at(rep, r0, nr):
        return pl.ds(pl.multiple_of(rep * rows + r0, 8), nr)

    def slot(p, rep):
        w, r0, nr, _ = pieces[p]
        return weights.at[w, rows_at(rep, r0, nr), :]

    half = feats // 2

    def feat_slot(s, h, block):
        return full.at[s, pl.ds(pl.multiple_of(block * feats + h * half, 8), half), :]

    def feat_sem(s, h, block):
        return x_sem.at[(s * 2 + h) * n_col + block]

    has_right, has_left = col < n_col - 1, col > 0
    right = {"col": jnp.minimum(col + 1, n_col - 1)}
    left = {"col": jnp.maximum(col - 1, 0)}

    def own_features(s):
        for h in range(2):
            src = streams[s].at[pl.ds(h * half, half), :]
            sends.start(src, feat_slot(s, h, col), feat_sem(s, h, col), right, has_right)
            sends.start(src, feat_slot(s, h, col), feat_sem(s, h, col), left, has_left)

    def own_weight(weight):
        for p, (w, r0, nr, route) in enumerate(pieces):
            if w != weight:
                continue
            src = mine[w].at[pl.ds(r0, nr), :]
            sem = w_sem.at[p * peers * 2 + me]
            for dq in range(1, nq):
                sends.start(src, slot(p, me), sem, q_peer(dq))
            for dy in range(1, ny):
                sends.start(src, slot(p, me), sem, y_peer(dy))
            sends.start(src, slot(p, me), sem, partner)

    own_features(0)
    own_weight(0)
    own_weight(1)
    locals_ = []
    for i, (src, dst) in enumerate(
        [(streams[s], full.at[s, pl.ds(pl.multiple_of(col * feats, 8), feats), :]) for s in range(2)]
        + [(mine[w], weights.at[w, rows_at(me, 0, rows), :]) for w in range(3)]
    ):
        locals_.append(pltpu.make_async_copy(src, dst, own_sem.at[i]))
        locals_[-1].start()

    def chain(s, step):
        from_left, from_right = col >= step, col + step < n_col
        lb, rb = jnp.maximum(col - step, 0), jnp.minimum(col + step, n_col - 1)
        for h in range(2):
            l_slot, l_sem = feat_slot(s, h, lb), feat_sem(s, h, lb)
            r_slot, r_sem = feat_slot(s, h, rb), feat_sem(s, h, rb)
            guarded(from_left, lambda: arrived(l_slot, l_sem))
            if step < n_col - 1:
                sends.start(l_slot, l_slot, l_sem, right, from_left & has_right)
            guarded(from_right, lambda: arrived(r_slot, r_sem))
            if step < n_col - 1:
                sends.start(r_slot, r_slot, r_sem, left, from_right & has_left)

    def take(p, rep, forward):
        sem = w_sem.at[p * peers * 2 + rep]
        arrived(slot(p, rep), sem)
        for where in forward + [partner]:
            sends.start(slot(p, rep), slot(p, rep), sem, where)

    def near(p):
        route = pieces[p][3]
        for dq in range(1, nq):
            take(p, rep_of(back_q(dq), c, y), [y_peer(i) for i in range(1, ny)] if route == 0 else [])
        for dy in range(1, ny):
            take(p, rep_of(q, c, back_y(dy)), [q_peer(i) for i in range(1, nq)] if route == 1 else [])

    def far(p):
        for dq in range(1, nq):
            for dy in range(1, ny):
                take(p, rep_of(back_q(dq), c, back_y(dy)), [])

    def from_partner(p):
        for dq in range(nq):
            for dy in range(ny):
                rep = rep_of(at_q(dq), 1 - c, at_y(dy))
                arrived(slot(p, rep), w_sem.at[p * peers * 2 + rep])

    near(0)
    chain(0, 1)
    near(1)
    own_weight(2)
    for step in range(2, n_col):
        if step == n_col - 1:
            own_features(1)
        chain(0, step)
    far(0)
    far(1)
    from_partner(0)
    from_partner(1)
    for copy in locals_:
        copy.wait()

    mt, nt = tile_of(toks, 256), tile_of(hid, 384)
    m_tiles, n_tiles = toks // mt, hid // nt
    token_dims = (((0,), (0,)), ((), ()))
    later = [p for p in range(len(pieces)) if pieces[p][0] == 2]

    def tile_slices(i):
        m, n = i // n_tiles, i % n_tiles
        return pl.ds(pl.multiple_of(m * mt, mt), mt), pl.ds(pl.multiple_of(n * nt, nt), nt)

    def project(first, last):
        @pl.loop(first, last)
        def _(i):
            ms, ns = tile_slices(i)
            x = full[0, :, ms]
            gate_pre = lax.dot_general(x, weights[0, :, ns], token_dims, preferred_element_type=F32)
            up_pre = lax.dot_general(x, weights[1, :, ns], token_dims, preferred_element_type=F32)
            act_val, slope_val = gelu_parts(gate_pre)
            grads[2, ms, ns] = (act_val * up_pre).astype(BF16)
            stash[0, ms, ns] = up_pre * slope_val
            stash[1, ms, ns] = act_val

    tiles = m_tiles * n_tiles
    project(0, tiles // 2)
    chain(1, 1)
    project(tiles // 2, tiles)
    for p in later:
        near(p)
    for step in range(2, n_col - 1):
        chain(1, step)

    def term(w, rep, ns):
        return jnp.dot(full[w // 2, rows_at(rep, 0, rows), :], grads[w, :, ns], preferred_element_type=F32)

    def n_slice(n):
        return pl.ds(pl.multiple_of(n * nt, nt), nt)

    def pair_copy(i):
        return pltpu.make_async_remote_copy(
            src_ref=partner_out.at[i],
            dst_ref=sums.at[i],
            send_sem=pair_send.at[i],
            recv_sem=pair_recv.at[i],
            device_id=partner,
            device_id_type=MESH,
        )

    def is_far(rep):
        block = (rep * rows) // feats
        return jnp.abs(block - col) == n_col - 1

    def partner_terms(w, when=None):
        @pl.loop(0, peers)
        def _(peer):
            i = w * peers + peer
            rep = rep_of(peer // ny, 1 - c, peer % ny)

            def one():
                @pl.loop(0, n_tiles)
                def _(n):
                    partner_out[i, :, n_slice(n)] = term(w, rep, n_slice(n)).astype(BF16)

                pair_copy(i).start()

            guarded(None if when is None else when(rep), one)

    first_base, count = [], 0
    for _, _, _, route in pieces:
        first_base.append(count)
        count += (nq - 1) * ny if route == 0 else (ny - 1) * nq
    second_base, count = [], 0
    for _, _, _, route in pieces:
        second_base.append(count)
        count += (ny - 1) if route == 0 else (nq - 1)

    def first_slot(p, dq, dy):
        k = first_base[p] + ((dq - 1) * ny + dy if pieces[p][3] == 0 else (dy - 1) * nq + dq)
        return first_in.at[k, pl.ds(0, pieces[p][2]), :], first_sem.at[k]

    def second_slot(p, d):
        k = second_base[p] + d - 1
        return second_in.at[k, pl.ds(0, pieces[p][2]), :], second_sem.at[k]

    def own_terms(w, when=None):
        for dq in others_first(nq):
            for dy in others_first(ny):
                index = w * peers + at_q(dq) * ny + at_y(dy)
                rep = rep_of(at_q(dq), c, at_y(dy))
                cond = None if when is None else when(rep)

                def one():
                    arrived(sums.at[index], pair_recv.at[index])

                    @pl.loop(0, n_tiles)
                    def _(n):
                        ns = n_slice(n)
                        sums[index, :, ns] = (term(w, rep, ns) + sums[index, :, ns].astype(F32)).astype(BF16)

                guarded(cond, one)
                for p, (pw, r0, nr, route) in enumerate(pieces):
                    if pw == w and (dq if route == 0 else dy):
                        dst, sem = first_slot(p, dq, dy)
                        where = q_peer(dq) if route == 0 else y_peer(dy)
                        sends.start(sums.at[index, pl.ds(r0, nr), :], dst, sem, where, cond)

    rt = tile_of(feats, 288)
    hid_dims = (((1,), (1,)), ((), ()))

    def input_part(dz):
        block = lax.rem(col + dz, n_col)

        @pl.loop(0, feats // rt)
        def _(r):
            rs = pl.ds(pl.multiple_of(block * feats + r * rt, 8), rt)
            part = lax.dot_general(weights[0, rs, :], grads[0], hid_dims, preferred_element_type=F32)
            part = part + lax.dot_general(weights[1, rs, :], grads[1], hid_dims, preferred_element_type=F32)
            ig_out[dz, pl.ds(pl.multiple_of(r * rt, 8), rt), :] = part.astype(BF16)

        if dz:
            sends.start(ig_out.at[dz], ig_in.at[dz - 1], ig_sem.at[dz - 1], {"col": block})

    outs = (og_ref, ou_ref, od_ref)

    def second(p):
        w, r0, nr, route = pieces[p]
        rs = pl.ds(r0, nr)
        n_first, n_second = (nq, ny) if route == 0 else (ny, nq)
        for d in others_first(n_second):
            index = w * peers + (q * ny + at_y(d) if route == 0 else at_q(d) * ny + y)
            total = sums[index, rs, :].astype(F32)
            for f in range(1, n_first):
                ref, sem = first_slot(p, f, d) if route == 0 else first_slot(p, d, f)
                arrived(ref, sem)
                total = total + ref[...].astype(F32)
            if d:
                sums[index, rs, :] = total.astype(BF16)
                dst, sem = second_slot(p, d)
                sends.start(sums.at[index, rs, :], dst, sem, y_peer(d) if route == 0 else q_peer(d))
            else:
                outs[w][rs, :] = total

    near_rep = lambda rep: jnp.logical_not(is_far(rep))
    partner_terms(2, near_rep)
    own_terms(2, near_rep)
    for p in later:
        far(p)
    for p in later:
        from_partner(p)
    chain(1, n_col - 1)
    partner_terms(2, is_far)

    @pl.loop(0, tiles)
    def _(i):
        ms, ns = tile_slices(i)
        hidden_grad = lax.dot_general(full[1, :, ms], weights[2, :, ns], token_dims, preferred_element_type=F32)
        grads[0, ms, ns] = (hidden_grad * stash[0, ms, ns]).astype(BF16)
        grads[1, ms, ns] = (hidden_grad * stash[1, ms, ns]).astype(BF16)

    own_terms(2, is_far)
    spare = list(range(1, n_col))
    partner_terms(0)
    partner_terms(1)
    input_part(spare.pop(0))
    own_terms(0)
    own_terms(1)
    while spare:
        input_part(spare.pop(0))
    for p in later:
        second(p)
    input_part(0)
    for p in range(len(pieces)):
        if p not in later:
            second(p)

    total = ig_out[0].astype(F32)
    for dz in range(1, n_col):
        arrived(ig_in.at[dz - 1], ig_sem.at[dz - 1])
        total = total + ig_in[dz - 1].astype(F32)
    ig_ref[...] = total.astype(BF16)

    for p, (w, r0, nr, route) in enumerate(pieces):
        rs = pl.ds(r0, nr)
        for d in range(1, ny if route == 0 else nq):
            ref, sem = second_slot(p, d)
            arrived(ref, sem)
            outs[w][rs, :] = outs[w][rs, :] + ref[...].astype(F32)

    sends.finish()

    @pl.loop(0, 3 * peers)
    def _(i):
        pair_copy(i).wait_send()


def body(n_dp, n_row, n_col, act_in, cot_out, w_gate, w_up, w_down):
    toks, feats = act_in.shape
    rows, hid = w_gate.shape
    sizes = (n_dp, n_row, n_col, rows, hid, feats, toks)
    nq, ny = n_dp // 2, n_row
    peers, reps, dim = nq * ny, n_dp * n_row, feats * n_col
    pieces = pieces_of(rows)
    firsts = sum((nq - 1) * ny if r == 0 else (ny - 1) * nq for _, _, _, r in pieces)
    seconds = sum((ny - 1) if r == 0 else (nq - 1) for _, _, _, r in pieces)
    near_far = sum((nq - 1) * (ny - 1) for _ in pieces)
    n_sends = 8 + 8 * (n_col - 2) + len(pieces) * (nq + ny - 1) + len(pieces) * (peers - 1) + near_far
    n_sends += 2 * firsts + seconds + n_col - 1
    any_spec, vmem_spec = pl.BlockSpec(memory_space=pl.ANY), pl.BlockSpec(memory_space=pltpu.VMEM)
    dma = lambda n: pltpu.SemaphoreType.DMA((max(n, 1),))
    wgrad = jax.ShapeDtypeStruct((rows, hid), F32)
    ig_t, gate_grad, up_grad, down_t = pl.pallas_call(
        functools.partial(kernel, sizes),
        out_shape=[jax.ShapeDtypeStruct((feats, toks), BF16), wgrad, wgrad, wgrad],
        in_specs=[any_spec] * 5,
        out_specs=[vmem_spec] * 4,
        scratch_shapes=[
            pltpu.VMEM((2, dim, toks), BF16),
            pltpu.VMEM((3, dim, hid), BF16),
            pltpu.VMEM((3, toks, hid), BF16),
            pltpu.VMEM((2, toks, hid), F32),
            pltpu.VMEM((3 * peers, rows, hid), BF16),
            pltpu.VMEM((3 * peers, rows, hid), BF16),
            pltpu.VMEM((max(firsts, 1), rows, hid), BF16),
            pltpu.VMEM((max(seconds, 1), rows, hid), BF16),
            pltpu.VMEM((n_col, feats, toks), BF16),
            pltpu.VMEM((max(n_col - 1, 1), feats, toks), BF16),
            dma(5), dma(n_sends), dma(len(pieces) * reps), dma(4 * n_col), dma(3 * peers), dma(3 * peers),
            dma(firsts), dma(seconds), dma(n_col - 1),
        ],
        compiler_params=pltpu.CompilerParams(
            collective_id=0, has_side_effects=True, vmem_limit_bytes=67043328
        ),
    )(act_in.T, cot_out.T, w_gate, w_up, w_down.T)
    norm_scale = 1.0 / math.sqrt(toks * n_dp * n_row)
    return (ig_t.T, gate_grad * norm_scale, up_grad * norm_scale, (down_t * norm_scale).T)


def solution(mesh):
    grid = P(("dp", "row"), "col")
    flipped = P("col", ("dp", "row"))
    return jax.shard_map(
        functools.partial(body, mesh.shape["dp"], mesh.shape["row"], mesh.shape["col"]),
        mesh=mesh,
        in_specs=(grid, grid, grid, grid, flipped),
        out_specs=(grid, grid, grid, flipped),
        check_vma=False,
    )
```
